32 devices in a mesh: rows: 8 (over z, y), grp: 4 (over x, core).
Axes of the slice: x: 2, y: 2, z: 4, core: 2. Of those that a mesh axis runs over, the one named last changes fastest.
Arguments:
- basis: float32 [32, 65536], P(None, ('rows', 'grp')), may hold values from -0.03125 to 0.03125, as said below
- core: float32 [32, 32], replicated, may hold values from -0.3 to 4
- snapshots: bfloat16 [4, 32, 65536], P(None, 'grp', 'rows'), may hold values from -16 to 16
Outputs:
- new_basis: float32 [32, 65536], P(None, ('rows', 'grp'))
- new_core: float32 [32, 32], replicated
- first_coeffs: float32 [4, 32, 32], replicated
The draws below stay inside these ranges and needn't reach their ends.
Inputs may be any that keep to these rules, and one draw needn't show every extreme that they name: `basis`: rows orthonormal up to float32 rounding.
All inputs are finite; a program needn't handle non-finite values.
Results may differ from the reference program's by a relative error of at most 0.0003.
Values may be sent and summed in bfloat16 or wider, within the bound.
A program may use at most 64 MiB of HBM per device.

```python
import jax
import jax.numpy as jnp
from jax import lax

RANK = 32
COLS = 32
BATCHES = 4
NDOF = 65536


def basis_rows(key):
    return jnp.clip(jax.random.normal(jax.random.fold_in(key, 11), (RANK, NDOF), jnp.float32), -4.0, 4.0)


def shared_row(key):
    return jnp.clip(jax.random.normal(jax.random.fold_in(key, 12), (1, NDOF), jnp.float32), -4.0, 4.0)


def cholesky_pass(vectors):
    gram = lax.dot_general(vectors, vectors, (((1,), (1,)), ((), ())), precision=lax.Precision.HIGHEST, preferred_element_type=jnp.float32)
    factor = jnp.linalg.cholesky(gram)
    return lax.linalg.triangular_solve(factor, vectors, left_side=True, lower=True)


def draw_basis(key, part):
    vectors = basis_rows(key)
    return cholesky_pass(cholesky_pass(vectors))


def draw_core(key, part):
    logs = jax.random.uniform(jax.random.fold_in(key, 21), (RANK,), jnp.float32, jnp.log(0.5), jnp.log(2.0))
    below = jax.random.uniform(jax.random.fold_in(key, 22), (RANK, RANK), jnp.float32, -0.3, 0.3)
    return jnp.diag(jnp.exp(logs)) + jnp.tril(below, -1)


def draw_snapshots(key, part):
    vectors = basis_rows(key)
    shared = shared_row(key)
    weights = jax.random.normal(jax.random.fold_in(key, 13), (BATCHES * COLS, RANK), jnp.float32)
    spread = jnp.exp(jax.random.uniform(jax.random.fold_in(key, 14), (1, RANK), jnp.float32, jnp.log(0.3), jnp.log(3.0)))
    position = jnp.arange(NDOF, dtype=jnp.float32) / (NDOF - 1.0)
    noise = jax.random.normal(jax.random.fold_in(key, 15), (BATCHES * COLS, NDOF), jnp.float32)
    ramp = 1.0 + 2.0 * position
    values = (jnp.dot(weights * spread, vectors) + 0.5 * shared + 2.0 * noise) / 4.0
    values = jnp.clip(values * ramp[None, :], -16.0, 16.0)
    return values.reshape(BATCHES, COLS, NDOF).astype(jnp.bfloat16)


def setup_inputs(seed: int = 0) -> dict:
    keys = jax.random.split(jax.random.key(seed), 4)
    basis = draw_basis(jax.random.fold_in(keys[3], 71), 0)
    core = draw_core(jax.random.fold_in(keys[3], 71), 0)
    snapshots = draw_snapshots(jax.random.fold_in(keys[3], 71), 0)
    return dict(basis=basis, core=core, snapshots=snapshots)


epsilon = 1e-06

def contract_rows(left, right):
    return lax.dot_general(left.astype(jnp.float32), right.astype(jnp.float32), (((1,), (1,)), ((), ())), precision=lax.Precision.HIGHEST, preferred_element_type=jnp.float32)

def matmul(left, right):
    return jnp.dot(left.astype(jnp.float32), right.astype(jnp.float32), precision=lax.Precision.HIGHEST, preferred_element_type=jnp.float32)

def lower_solve(factor, right):
    return lax.linalg.triangular_solve(factor, right, left_side=True, lower=True)

def small_update(core_now, total, lower):
    rank = core_now.shape[0]
    cols = lower.shape[0]
    top = jnp.concatenate([core_now, total], axis=1)
    bottom = jnp.concatenate([jnp.zeros((cols, rank), jnp.float32), lower.T], axis=1)
    stacked = jnp.concatenate([top, bottom], axis=0)
    moment = matmul(stacked, stacked.T)
    leading = moment[:, :rank]
    factor = jnp.linalg.cholesky(matmul(leading.T, leading))
    rotation = lower_solve(factor, leading.T).T
    fresh_core = jnp.linalg.cholesky(matmul(rotation.T, matmul(moment, rotation)))
    return (rotation, fresh_core)

def reference(basis, core, snapshots):
    basis_now = basis
    core_now = core
    rank = basis.shape[0]
    firsts = []
    for batch in range(BATCHES):
        raw = snapshots[batch].astype(jnp.float32)
        squares = lax.optimization_barrier(jnp.sum(raw * raw, axis=1))
        scaled = raw * lax.rsqrt(squares + epsilon)[:, None]
        first = contract_rows(basis_now, scaled)
        firsts.append(first)
        once = scaled - matmul(first.T, basis_now)
        second = contract_rows(basis_now, once)
        twice = once - matmul(second.T, basis_now)
        total = first + second
        gram = contract_rows(twice, twice)
        lower = jnp.linalg.cholesky(gram)
        fresh = lower_solve(lower, twice)
        rotation, core_now = small_update(core_now, total, lower)
        basis_now = matmul(rotation[:rank].T, basis_now) + matmul(rotation[rank:].T, fresh)
    return (basis_now, core_now, jnp.stack(firsts, axis=0))
```

```python
import functools

import jax
import jax.numpy as jnp
from jax import lax
from jax.experimental import pallas as pl
from jax.experimental.pallas import tpu as pltpu
from jax.sharding import PartitionSpec as P

epsilon = 1e-06
BLOCK_ROWS = 8
MESH = pl.DeviceIdType.MESH


def mm(left, right):
    return lax.dot_general(
        left, right, (((1,), (0,)), ((), ())), precision=lax.Precision.HIGHEST, preferred_element_type=jnp.float32
    )


def mt(left, right):
    return lax.dot_general(
        left, right, (((1,), (1,)), ((), ())), precision=lax.Precision.HIGHEST, preferred_element_type=jnp.float32
    )


def split(x):
    high = x.astype(jnp.bfloat16)
    rest = x - high.astype(jnp.float32)
    mid = rest.astype(jnp.bfloat16)
    low = (rest - mid.astype(jnp.float32)).astype(jnp.bfloat16)
    return high, mid, low


def gram_kernel(
    nrows, ngrp, basis_ref, snap_ref, z_ref, sum_ref,
    raw, basis_v, z, part, landed, crossed, total,
    basis_sem, own_sem, z_sem, a2a_send, a2a_recv, rs_send, rs_recv, x_send, x_recv, ag_send, ag_recv,
):
    row, grp = lax.axis_index("rows"), lax.axis_index("grp")
    rank, width = basis_ref.shape
    members = BLOCK_ROWS * ngrp
    blocks = nrows // BLOCK_ROWS
    block = row // BLOCK_ROWS
    me = (row % BLOCK_ROWS) * ngrp + grp

    def device(q):
        return (block * BLOCK_ROWS + q // ngrp, q % ngrp)

    def peer(step):
        return lax.rem(me + step, members)

    def other(step):
        return (lax.rem(block + step, blocks) * BLOCK_ROWS + row % BLOCK_ROWS, grp)

    def piece(g):
        return snap_ref.at[:, :, pl.ds(pl.multiple_of(g * width, 128), width)]

    load_basis = pltpu.make_async_copy(basis_ref, basis_v, basis_sem)
    load_basis.start()
    load_own = pltpu.make_async_copy(piece(grp), raw.at[:, grp], own_sem)
    load_own.start()

    barrier = pltpu.get_barrier_semaphore()

    @pl.loop(1, members)
    def _(step):
        pl.semaphore_signal(barrier, inc=1, device_id=device(peer(step)), device_id_type=MESH)

    if blocks > 1:

        @pl.loop(1, blocks)
        def _(step):
            pl.semaphore_signal(barrier, inc=1, device_id=other(step), device_id_type=MESH)

    pl.semaphore_wait(barrier, members - 1 + blocks - 1)

    sends = []
    for step in range(1, ngrp):
        target = lax.rem(grp + step, ngrp)
        copy = pltpu.make_async_remote_copy(
            src_ref=piece(target), dst_ref=raw.at[:, grp],
            send_sem=a2a_send.at[step - 1], recv_sem=a2a_recv.at[step - 1],
            device_id=(row, target), device_id_type=MESH,
        )
        copy.start()
        sends.append(copy)

    load_basis.wait()
    high, mid, low = split(basis_v[...])
    columns = raw.shape[0] * raw.shape[1] * raw.shape[2]
    z[columns:columns + rank, :] = high
    z[columns + rank:columns + 2 * rank, :] = mid
    z[columns + 2 * rank:, :] = low
    load_own.wait()
    for copy in sends:
        copy.wait()
    z[:columns, :] = raw[...].astype(jnp.float32).reshape(columns, width).astype(jnp.bfloat16)
    store_z = pltpu.make_async_copy(z, z_ref, z_sem)
    store_z.start()
    zz = z[...]
    full = lax.dot_general(zz, zz, (((1,), (1,)), ((), ())), preferred_element_type=jnp.float32)
    basis_rows = full[columns:columns + rank] + full[columns + rank:columns + 2 * rank] + full[columns + 2 * rank:]
    cross = basis_rows[:, :columns]
    tail = jnp.concatenate([basis_rows[:, columns:], jnp.zeros((rank, columns - 3 * rank), jnp.float32)], axis=1)
    inner = tail + pltpu.roll(tail, columns - rank, 1) + pltpu.roll(tail, columns - 2 * rank, 1)
    lane = lax.broadcasted_iota(jnp.int32, (rank, columns), 1)
    first = full[:rank, :columns]
    second = jnp.where(lane < rank, inner, full[rank:2 * rank, :columns])
    last = pltpu.roll(full[3 * rank:4 * rank, :columns], rank, 1)
    third = jnp.where(lane < rank, last, full[2 * rank:3 * rank, :columns])
    size = part.shape[1]
    for i, value in enumerate((cross, first, second, third)):
        for j in range(rank // size):
            part[i * (rank // size) + j] = value[j * size:(j + 1) * size]

    @pl.loop(1, members)
    def _(step):
        target = peer(step)
        pltpu.make_async_remote_copy(
            src_ref=part.at[target], dst_ref=landed.at[step - 1],
            send_sem=rs_send, recv_sem=rs_recv, device_id=device(target), device_id_type=MESH,
        ).start()

    pltpu.make_async_copy(landed, landed, rs_recv).wait()
    mine = part[me] + jnp.sum(landed[...], axis=0)
    if blocks > 1:
        crossed[0] = mine

        @pl.loop(1, blocks)
        def _(step):
            pltpu.make_async_remote_copy(
                src_ref=crossed.at[0], dst_ref=crossed.at[step],
                send_sem=x_send, recv_sem=x_recv, device_id=other(step), device_id_type=MESH,
            ).start()

        rest = crossed.at[pl.ds(1, blocks - 1)]
        pltpu.make_async_copy(rest, rest, x_recv).wait()
        mine = jnp.sum(crossed[...], axis=0)
    total[me] = mine

    @pl.loop(1, members)
    def _(step):
        pltpu.make_async_remote_copy(
            src_ref=total.at[me], dst_ref=total.at[me],
            send_sem=ag_send, recv_sem=ag_recv, device_id=device(peer(step)), device_id_type=MESH,
        ).start()

    most = total.at[pl.ds(0, members - 1)]
    pltpu.make_async_copy(most, most, ag_recv).wait()
    for j in range(members):
        sum_ref[j * size:(j + 1) * size, :] = total[j]
    pltpu.make_async_copy(landed, landed, rs_send).wait()
    if blocks > 1:
        pltpu.make_async_copy(rest, rest, x_send).wait()
    pltpu.make_async_copy(most, most, ag_send).wait()
    store_z.wait()


def eliminate(matrix):
    n = matrix.shape[0]
    r = lax.broadcasted_iota(jnp.int32, (n, 1), 0)
    c = lax.broadcasted_iota(jnp.int32, (n, n), 1)
    eye = (c == lax.broadcasted_iota(jnp.int32, (n, n), 0)).astype(jnp.float32)
    work = jnp.concatenate([matrix, eye], axis=1)
    for k in range(n):
        row = work[k:k + 1, :]
        pivot = work[k:k + 1, k:k + 1]
        column = work[:, k:k + 1]
        factor = jnp.where(r > k, column / pivot, 0.0)
        work = jnp.where(r == k, work * lax.rsqrt(pivot), work - factor * row)
    return work[:, :n], work[:, n:]


def update_kernel(batches, sum_ref, core_ref, z_ref, basis_out, core_out, first_out, z, z_sem):
    load = pltpu.make_async_copy(z_ref, z, z_sem)
    load.start()
    rank = core_ref.shape[0]
    width = sum_ref.shape[1]
    lane = lax.broadcasted_iota(jnp.int32, (rank, width), 1)
    sub = lax.broadcasted_iota(jnp.int32, (rank, width), 0)
    kept = [sum_ref[rank * (1 + b):rank * (2 + b), :] for b in range(batches - 1)]
    kept.append(pltpu.roll(kept[-1], width - rank, 1))
    picks = [jnp.where(lane == sub + rank * b, kept[b], 0.0) for b in range(batches)]
    inverse_row = lax.rsqrt(jnp.sum(sum(picks), axis=0, keepdims=True) + epsilon)
    inverse_cols = [lax.rsqrt(jnp.sum(p, axis=1, keepdims=True) + epsilon) for p in picks]
    grams = [kept[b] * inverse_cols[b] * inverse_row for b in range(batches)]
    gram_basis = sum_ref[2 * rank:3 * rank, :rank]
    hits = sum_ref[:rank, :] * inverse_row
    coef_basis = (lane[:, :rank] == sub[:, :rank]).astype(jnp.float32)
    coef_raw = jnp.zeros((rank, width), jnp.float32)
    core = core_ref[...]
    energy = mt(core, core)
    for b in range(batches):
        cross = hits[:, b * rank:(b + 1) * rank]
        first_out[b] = cross
        total = cross + (cross - mm(gram_basis, cross))
        w1 = mm(energy, gram_basis) + mt(total, cross)
        w2 = mm(energy, cross) + mm(total, grams[b][:, b * rank:(b + 1) * rank])
        square = mt(w1, energy) + mt(w2, total)
        placed = [total]
        if b > 0:
            placed.insert(0, jnp.zeros((rank, b * rank), jnp.float32))
        if b < batches - 1:
            placed.append(jnp.zeros((rank, width - (b + 1) * rank), jnp.float32))
        v_basis = mm(energy, coef_basis)
        v_raw = mm(energy, coef_raw) + jnp.concatenate(placed, axis=1)
        v_hits = mm(energy, hits) + mm(total, grams[b])
        _, inverse = eliminate(square)
        coef_basis = mm(inverse, v_basis)
        coef_raw = mm(inverse, v_raw)
        hits = mm(inverse, v_hits)
        n1 = mm(inverse, w1)
        n2 = mm(inverse, w2)
        gram_basis = mt(mm(inverse, square), inverse)
        energy = mt(mm(n1, energy), n1) + mt(n2, n2)
    upper, _ = eliminate(energy)
    keep = lax.broadcasted_iota(jnp.int32, (rank, rank), 0) <= lax.broadcasted_iota(jnp.int32, (rank, rank), 1)
    core_out[...] = jnp.where(keep, upper, 0.0).T
    coef = jnp.concatenate([coef_raw * inverse_row] + [coef_basis] * 3, axis=1)
    pieces = jnp.concatenate([p.astype(jnp.float32) for p in split(coef)], axis=0).astype(jnp.bfloat16)
    load.wait()
    wide = jnp.dot(pieces, z[...], preferred_element_type=jnp.float32)
    basis_out[...] = wide[:rank] + wide[rank:2 * rank] + wide[2 * rank:]


def solution(mesh):
    nrows, ngrp = mesh.shape["rows"], mesh.shape["grp"]

    def body(basis, core, snapshots):
        rank, width = basis.shape
        batches, cols, _ = snapshots.shape
        columns = batches * cols * ngrp
        height = columns + 3 * rank
        members = BLOCK_ROWS * ngrp
        blocks = nrows // BLOCK_ROWS
        size = batches * rank // members
        vmem = pl.BlockSpec(memory_space=pltpu.VMEM)
        hbm = pl.BlockSpec(memory_space=pl.ANY)
        dma = pltpu.SemaphoreType.DMA
        z, sums = pl.pallas_call(
            functools.partial(gram_kernel, nrows, ngrp),
            out_shape=(
                jax.ShapeDtypeStruct((height, width), jnp.bfloat16),
                jax.ShapeDtypeStruct((batches * rank, columns), jnp.float32),
            ),
            in_specs=[hbm, hbm],
            out_specs=(hbm, vmem),
            scratch_shapes=[
                pltpu.VMEM((batches, ngrp, cols, width), jnp.bfloat16),
                pltpu.VMEM((rank, width), jnp.float32),
                pltpu.VMEM((height, width), jnp.bfloat16),
                pltpu.VMEM((members, size, columns), jnp.float32),
                pltpu.VMEM((members - 1, size, columns), jnp.float32),
                pltpu.VMEM((blocks, size, columns), jnp.float32),
                pltpu.VMEM((members, size, columns), jnp.float32),
                dma, dma, dma, dma((ngrp - 1,)), dma((ngrp - 1,)),
                dma, dma, dma, dma, dma, dma,
            ],
            compiler_params=pltpu.CompilerParams(collective_id=0, has_side_effects=True),
        )(basis, snapshots)
        return pl.pallas_call(
            functools.partial(update_kernel, batches),
            out_shape=(
                jax.ShapeDtypeStruct((rank, width), jnp.float32),
                jax.ShapeDtypeStruct((rank, rank), jnp.float32),
                jax.ShapeDtypeStruct((batches, rank, rank), jnp.float32),
            ),
            in_specs=[vmem, vmem, hbm],
            out_specs=(vmem, vmem, vmem),
            scratch_shapes=[pltpu.VMEM((height, width), jnp.bfloat16), dma],
        )(sums, core, z)

    return jax.shard_map(
        body,
        mesh=mesh,
        in_specs=(P(None, ("rows", "grp")), P(), P(None, "grp", "rows")),
        out_specs=(P(None, ("rows", "grp")), P(), P()),
        check_vma=False,
    )
```

```python
import functools

import jax
import jax.numpy as jnp
from jax import lax
from jax.experimental import pallas as pl
from jax.experimental.pallas import tpu as pltpu
from jax.sharding import PartitionSpec as P

epsilon = 1e-06
BLOCK_ROWS = 8
MESH = pl.DeviceIdType.MESH


def mm(left, right):
    return lax.dot_general(
        left, right, (((1,), (0,)), ((), ())), precision=lax.Precision.HIGHEST, preferred_element_type=jnp.float32
    )


def mt(left, right):
    return lax.dot_general(
        left, right, (((1,), (1,)), ((), ())), precision=lax.Precision.HIGHEST, preferred_element_type=jnp.float32
    )


def split(x):
    high = x.astype(jnp.bfloat16)
    rest = x - high.astype(jnp.float32)
    mid = rest.astype(jnp.bfloat16)
    low = (rest - mid.astype(jnp.float32)).astype(jnp.bfloat16)
    return high, mid, low


def gram_kernel(
    nrows, ngrp, basis_ref, snap_ref, z_ref, sum_ref,
    raw, basis_v, z, part, landed, crossed, total,
    basis_sem, own_sem, z_sem, a2a_send, a2a_recv, rs_send, rs_recv, x_send, x_recv, ag_send, ag_recv,
):
    row, grp = lax.axis_index("rows"), lax.axis_index("grp")
    rank, width = basis_ref.shape
    members = BLOCK_ROWS * ngrp
    blocks = nrows // BLOCK_ROWS
    block = row // BLOCK_ROWS
    me = (row % BLOCK_ROWS) * ngrp + grp

    def device(q):
        return (block * BLOCK_ROWS + q // ngrp, q % ngrp)

    def peer(step):
        return lax.rem(me + step, members)

    def other(step):
        return (lax.rem(block + step, blocks) * BLOCK_ROWS + row % BLOCK_ROWS, grp)

    def piece(g):
        return snap_ref.at[:, :, pl.ds(pl.multiple_of(g * width, 128), width)]

    load_basis = pltpu.make_async_copy(basis_ref, basis_v, basis_sem)
    load_basis.start()
    load_own = pltpu.make_async_copy(piece(grp), raw.at[:, grp], own_sem)
    load_own.start()

    barrier = pltpu.get_barrier_semaphore()

    @pl.loop(1, members)
    def _(step):
        pl.semaphore_signal(barrier, inc=1, device_id=device(peer(step)), device_id_type=MESH)

    if blocks > 1:

        @pl.loop(1, blocks)
        def _(step):
            pl.semaphore_signal(barrier, inc=1, device_id=other(step), device_id_type=MESH)

    pl.semaphore_wait(barrier, members - 1 + blocks - 1)

    sends = []
    for step in range(1, ngrp):
        target = lax.rem(grp + step, ngrp)
        copy = pltpu.make_async_remote_copy(
            src_ref=piece(target), dst_ref=raw.at[:, grp],
            send_sem=a2a_send.at[step - 1], recv_sem=a2a_recv.at[step - 1],
            device_id=(row, target), device_id_type=MESH,
        )
        copy.start()
        sends.append(copy)

    load_basis.wait()
    high, mid, low = split(basis_v[...])
    columns = raw.shape[0] * raw.shape[1] * raw.shape[2]
    z[columns:columns + rank, :] = high
    z[columns + rank:columns + 2 * rank, :] = mid
    z[columns + 2 * rank:, :] = low
    load_own.wait()
    for copy in sends:
        copy.wait()
    z[:columns, :] = raw[...].astype(jnp.float32).reshape(columns, width).astype(jnp.bfloat16)
    store_z = pltpu.make_async_copy(z, z_ref, z_sem)
    store_z.start()
    zz = z[...]
    full = lax.dot_general(zz, zz, (((1,), (1,)), ((), ())), preferred_element_type=jnp.float32)
    basis_rows = full[columns:columns + rank] + full[columns + rank:columns + 2 * rank] + full[columns + 2 * rank:]
    cross = basis_rows[:, :columns]
    tail = jnp.concatenate([basis_rows[:, columns:], jnp.zeros((rank, columns - 3 * rank), jnp.float32)], axis=1)
    inner = tail + pltpu.roll(tail, columns - rank, 1) + pltpu.roll(tail, columns - 2 * rank, 1)
    lane = lax.broadcasted_iota(jnp.int32, (rank, columns), 1)
    first = full[:rank, :columns]
    second = jnp.where(lane < rank, inner, full[rank:2 * rank, :columns])
    last = pltpu.roll(full[3 * rank:4 * rank, :columns], rank, 1)
    third = jnp.where(lane < rank, last, full[2 * rank:3 * rank, :columns])
    size = part.shape[1]
    for i, value in enumerate((cross, first, second, third)):
        for j in range(rank // size):
            part[i * (rank // size) + j] = value[j * size:(j + 1) * size]

    @pl.loop(1, members)
    def _(step):
        target = peer(step)
        pltpu.make_async_remote_copy(
            src_ref=part.at[target], dst_ref=landed.at[step - 1],
            send_sem=rs_send, recv_sem=rs_recv, device_id=device(target), device_id_type=MESH,
        ).start()

    pltpu.make_async_copy(landed, landed, rs_recv).wait()
    mine = part[me] + jnp.sum(landed[...], axis=0)
    if blocks > 1:
        crossed[0] = mine

        @pl.loop(1, blocks)
        def _(step):
            pltpu.make_async_remote_copy(
                src_ref=crossed.at[0], dst_ref=crossed.at[step],
                send_sem=x_send, recv_sem=x_recv, device_id=other(step), device_id_type=MESH,
            ).start()

        rest = crossed.at[pl.ds(1, blocks - 1)]
        pltpu.make_async_copy(rest, rest, x_recv).wait()
        mine = jnp.sum(crossed[...], axis=0)
    total[me] = mine

    @pl.loop(1, members)
    def _(step):
        pltpu.make_async_remote_copy(
            src_ref=total.at[me], dst_ref=total.at[me],
            send_sem=ag_send, recv_sem=ag_recv, device_id=device(peer(step)), device_id_type=MESH,
        ).start()

    most = total.at[pl.ds(0, members - 1)]
    pltpu.make_async_copy(most, most, ag_recv).wait()
    for j in range(members):
        sum_ref[j * size:(j + 1) * size, :] = total[j]
    pltpu.make_async_copy(landed, landed, rs_send).wait()
    if blocks > 1:
        pltpu.make_async_copy(rest, rest, x_send).wait()
    pltpu.make_async_copy(most, most, ag_send).wait()
    store_z.wait()


def eliminate(matrix, want_lower=False):
    n = matrix.shape[0]
    tile = 8
    tiles = n // tile
    r = lax.broadcasted_iota(jnp.int32, (tile, n), 0)
    c = lax.broadcasted_iota(jnp.int32, (tile, n), 1)
    left = [matrix[t * tile:(t + 1) * tile] for t in range(tiles)]
    if want_lower:
        result = [jnp.zeros((tile, n), jnp.float32)] * tiles
    else:
        result = [(c == r + t * tile).astype(jnp.float32) for t in range(tiles)]
    for t in range(tiles):
        below = range(t, tiles)
        panel = [
            {u: jnp.broadcast_to(left[u][:, t * tile + j:t * tile + j + 1], (tile, n)) for u in below}
            for j in range(tile)
        ]
        scale = jnp.ones((tile, n), jnp.float32)
        for j in range(tile):
            k = t * tile + j
            column = panel[j]
            pivot = column[t][j:j + 1]
            inverse = 1.0 / pivot
            root = lax.rsqrt(pivot)
            if want_lower:
                for u in below:
                    keep = (c == k) & (r >= j) if u == t else c == k
                    result[u] = jnp.where(keep, column[u] * root, result[u])
            else:
                scale = jnp.where(r == j, root, scale)
            masked = {u: jnp.where(r > j, column[u], 0.0) if u == t else column[u] for u in below}
            for l in range(j + 1, tile):
                head = panel[l][t][j:j + 1]
                for u in below:
                    panel[l][u] = panel[l][u] - (masked[u] * head) * inverse
            top = left[t][j:j + 1] * inverse
            body = result[t][j:j + 1] * inverse
            for u in below:
                if t < tiles - 1:
                    left[u] = left[u] - masked[u] * top
                if not want_lower:
                    result[u] = result[u] - masked[u] * body
        if not want_lower:
            result[t] = result[t] * scale
    return jnp.concatenate(result, axis=0)


def update_kernel(batches, sum_ref, core_ref, z_ref, basis_out, core_out, first_out, z, z_sem):
    load = pltpu.make_async_copy(z_ref, z, z_sem)
    load.start()
    rank = core_ref.shape[0]
    width = sum_ref.shape[1]
    lane = lax.broadcasted_iota(jnp.int32, (rank, width), 1)
    sub = lax.broadcasted_iota(jnp.int32, (rank, width), 0)
    kept = [sum_ref[rank * (1 + b):rank * (2 + b), :] for b in range(batches - 1)]
    kept.append(pltpu.roll(kept[-1], width - rank, 1))
    picks = [jnp.where(lane == sub + rank * b, kept[b], 0.0) for b in range(batches)]
    inverse_row = lax.rsqrt(jnp.sum(sum(picks), axis=0, keepdims=True) + epsilon)
    inverse_cols = [lax.rsqrt(jnp.sum(p, axis=1, keepdims=True) + epsilon) for p in picks]
    grams = [kept[b] * inverse_cols[b] * inverse_row for b in range(batches)]
    gram_basis = sum_ref[2 * rank:3 * rank, :rank]
    hits = sum_ref[:rank, :] * inverse_row
    coef_basis = (lane[:, :rank] == sub[:, :rank]).astype(jnp.float32)
    coef_raw = jnp.zeros((rank, width), jnp.float32)
    core = core_ref[...]
    energy = mt(core, core)
    for b in range(batches):
        cross = hits[:, b * rank:(b + 1) * rank]
        first_out[b] = cross
        total = cross + (cross - mm(gram_basis, cross))
        w1 = mm(energy, gram_basis) + mt(total, cross)
        w2 = mm(energy, cross) + mm(total, grams[b][:, b * rank:(b + 1) * rank])
        w1_energy = mm(w1, energy)
        square = w1_energy + mt(w2, total)
        placed = [total]
        if b > 0:
            placed.insert(0, jnp.zeros((rank, b * rank), jnp.float32))
        if b < batches - 1:
            placed.append(jnp.zeros((rank, width - (b + 1) * rank), jnp.float32))
        v_basis = mm(energy, coef_basis)
        v_raw = mm(energy, coef_raw) + jnp.concatenate(placed, axis=1)
        v_hits = mm(energy, hits) + mm(total, grams[b])
        inverse = eliminate(square)
        coef_basis = mm(inverse, v_basis)
        coef_raw = mm(inverse, v_raw)
        hits = mm(inverse, v_hits)
        n1 = mm(inverse, w1)
        n2 = mm(inverse, w2)
        gram_basis = mt(mm(inverse, square), inverse)
        energy = mt(mm(inverse, w1_energy), n1) + mt(n2, n2)
    coef = jnp.concatenate([coef_raw * inverse_row] + [coef_basis] * 3, axis=1)
    pieces = jnp.concatenate([p.astype(jnp.float32) for p in split(coef)], axis=0).astype(jnp.bfloat16)
    load.wait()
    wide = jnp.dot(pieces, z[...], preferred_element_type=jnp.float32)
    core_out[...] = eliminate(energy, want_lower=True)
    basis_out[...] = wide[:rank] + wide[rank:2 * rank] + wide[2 * rank:]


def solution(mesh):
    nrows, ngrp = mesh.shape["rows"], mesh.shape["grp"]

    def body(basis, core, snapshots):
        rank, width = basis.shape
        batches, cols, _ = snapshots.shape
        columns = batches * cols * ngrp
        height = columns + 3 * rank
        members = BLOCK_ROWS * ngrp
        blocks = nrows // BLOCK_ROWS
        size = batches * rank // members
        vmem = pl.BlockSpec(memory_space=pltpu.VMEM)
        hbm = pl.BlockSpec(memory_space=pl.ANY)
        dma = pltpu.SemaphoreType.DMA
        z, sums = pl.pallas_call(
            functools.partial(gram_kernel, nrows, ngrp),
            out_shape=(
                jax.ShapeDtypeStruct((height, width), jnp.bfloat16),
                jax.ShapeDtypeStruct((batches * rank, columns), jnp.float32),
            ),
            in_specs=[hbm, hbm],
            out_specs=(hbm, vmem),
            scratch_shapes=[
                pltpu.VMEM((batches, ngrp, cols, width), jnp.bfloat16),
                pltpu.VMEM((rank, width), jnp.float32),
                pltpu.VMEM((height, width), jnp.bfloat16),
                pltpu.VMEM((members, size, columns), jnp.float32),
                pltpu.VMEM((members - 1, size, columns), jnp.float32),
                pltpu.VMEM((blocks, size, columns), jnp.float32),
                pltpu.VMEM((members, size, columns), jnp.float32),
                dma, dma, dma, dma((ngrp - 1,)), dma((ngrp - 1,)),
                dma, dma, dma, dma, dma, dma,
            ],
            compiler_params=pltpu.CompilerParams(collective_id=0, has_side_effects=True),
        )(basis, snapshots)
        return pl.pallas_call(
            functools.partial(update_kernel, batches),
            out_shape=(
                jax.ShapeDtypeStruct((rank, width), jnp.float32),
                jax.ShapeDtypeStruct((rank, rank), jnp.float32),
                jax.ShapeDtypeStruct((batches, rank, rank), jnp.float32),
            ),
            in_specs=[vmem, vmem, hbm],
            out_specs=(vmem, vmem, vmem),
            scratch_shapes=[pltpu.VMEM((height, width), jnp.bfloat16), dma],
        )(sums, core, z)

    return jax.shard_map(
        body,
        mesh=mesh,
        in_specs=(P(None, ("rows", "grp")), P(), P(None, "grp", "rows")),
        out_specs=(P(None, ("rows", "grp")), P(), P()),
        check_vma=False,
    )
```

```python
import functools

import jax
import jax.numpy as jnp
from jax import lax
from jax.experimental import pallas as pl
from jax.experimental.pallas import tpu as pltpu
from jax.sharding import PartitionSpec as P

epsilon = 1e-06
BLOCK_ROWS = 8
STAGES = ((0, 1), (1, 2), (2, 4))
GROUPS = (1, 1, 3)
MESH = pl.DeviceIdType.MESH


def mm(left, right):
    return lax.dot_general(
        left, right, (((1,), (0,)), ((), ())), precision=lax.Precision.HIGHEST, preferred_element_type=jnp.float32
    )


def mt(left, right):
    return lax.dot_general(
        left, right, (((1,), (1,)), ((), ())), precision=lax.Precision.HIGHEST, preferred_element_type=jnp.float32
    )


def split(x):
    high = x.astype(jnp.bfloat16)
    rest = x - high.astype(jnp.float32)
    mid = rest.astype(jnp.bfloat16)
    low = (rest - mid.astype(jnp.float32)).astype(jnp.bfloat16)
    return high, mid, low


def eliminate(matrix, want_lower=False):
    n = matrix.shape[0]
    tile = 8
    tiles = n // tile
    r = lax.broadcasted_iota(jnp.int32, (tile, n), 0)
    c = lax.broadcasted_iota(jnp.int32, (tile, n), 1)
    left = [matrix[t * tile:(t + 1) * tile] for t in range(tiles)]
    if want_lower:
        result = [jnp.zeros((tile, n), jnp.float32)] * tiles
    else:
        result = [(c == r + t * tile).astype(jnp.float32) for t in range(tiles)]
    for t in range(tiles):
        below = range(t, tiles)
        panel = [
            {u: jnp.broadcast_to(left[u][:, t * tile + j:t * tile + j + 1], (tile, n)) for u in below}
            for j in range(tile)
        ]
        scale = jnp.ones((tile, n), jnp.float32)
        for j in range(tile):
            k = t * tile + j
            column = panel[j]
            pivot = column[t][j:j + 1]
            inverse = 1.0 / pivot
            root = lax.rsqrt(pivot)
            if want_lower:
                for u in below:
                    keep = (c == k) & (r >= j) if u == t else c == k
                    result[u] = jnp.where(keep, column[u] * root, result[u])
            else:
                scale = jnp.where(r == j, root, scale)
            masked = {u: jnp.where(r > j, column[u], 0.0) if u == t else column[u] for u in below}
            for l in range(j + 1, tile):
                head = panel[l][t][j:j + 1]
                for u in below:
                    panel[l][u] = panel[l][u] - (masked[u] * head) * inverse
            top = left[t][j:j + 1] * inverse
            body = result[t][j:j + 1] * inverse
            for u in below:
                if t < tiles - 1:
                    left[u] = left[u] - masked[u] * top
                if not want_lower:
                    result[u] = result[u] - masked[u] * body
        if not want_lower:
            result[t] = result[t] * scale
    return jnp.concatenate(result, axis=0)


def fused_kernel(nrows, ngrp, basis_ref, core_ref, snap_ref, z_ref, coef_ref, energy_ref, first_ref, raw, basis_v, z, *scratch):
    count = len(STAGES)
    parts, landeds, crosseds, totals = (scratch[i * count:(i + 1) * count] for i in range(4))
    basis_sem, own_sem, z_sem, a2a_send, a2a_recv, rs_send, rs_recv, x_send, x_recv, ag_send, ag_recv = scratch[4 * count:]
    row, grp = lax.axis_index("rows"), lax.axis_index("grp")
    rank, width = basis_ref.shape
    batches, cols, _ = snap_ref.shape
    members = BLOCK_ROWS * ngrp
    blocks = nrows // BLOCK_ROWS
    block = row // BLOCK_ROWS
    me = (row % BLOCK_ROWS) * ngrp + grp

    def device(q):
        return (block * BLOCK_ROWS + q // ngrp, q % ngrp)

    def peer(step):
        return lax.rem(me + step, members)

    def other(step):
        return (lax.rem(block + step, blocks) * BLOCK_ROWS + row % BLOCK_ROWS, grp)

    def piece(g, start, stop):
        return snap_ref.at[start:stop, :, pl.ds(pl.multiple_of(g * width, 128), width)]

    load_basis = pltpu.make_async_copy(basis_ref, basis_v, basis_sem)
    load_basis.start()
    load_own = pltpu.make_async_copy(piece(grp, 0, batches), raw.at[:, grp], own_sem)
    load_own.start()

    barrier = pltpu.get_barrier_semaphore()

    @pl.loop(1, members)
    def _(step):
        pl.semaphore_signal(barrier, inc=1, device_id=device(peer(step)), device_id_type=MESH)

    if blocks > 1:

        @pl.loop(1, blocks)
        def _(step):
            pl.semaphore_signal(barrier, inc=1, device_id=other(step), device_id_type=MESH)

    pl.semaphore_wait(barrier, members - 1 + blocks - 1)

    sends = []
    for s, (start, stop) in enumerate(STAGES):
        stage = []
        for step in range(1, ngrp):
            target = lax.rem(grp + step, ngrp)
            copy = pltpu.make_async_remote_copy(
                src_ref=piece(target, start, stop), dst_ref=raw.at[start:stop, grp],
                send_sem=a2a_send.at[s, step - 1], recv_sem=a2a_recv.at[s, step - 1],
                device_id=(row, target), device_id_type=MESH,
            )
            copy.start()
            stage.append(copy)
        sends.append(stage)

    load_basis.wait()
    base = 3 * rank
    for i, value in enumerate(split(basis_v[...])):
        z[i * rank:(i + 1) * rank, :] = value
    load_own.wait()
    lane = lax.broadcasted_iota(jnp.int32, (rank, 4 * rank), 1)

    def products(left, right):
        return lax.dot_general(left, right, (((1,), (1,)), ((), ())), preferred_element_type=jnp.float32)

    def fold(x):
        return x + pltpu.roll(x, 3 * rank, 1) + pltpu.roll(x, 2 * rank, 1)

    def widen(x):
        missing = 4 * rank - x.shape[1]
        return x if missing == 0 else jnp.concatenate([x, jnp.zeros((rank, missing), jnp.float32)], axis=1)

    inner = products(z[:base, :], z[:base, :])
    inner = widen(inner[:rank] + inner[rank:2 * rank] + inner[2 * rank:])
    inner = pltpu.roll(fold(inner), rank, 1)

    def reduce_start(s):
        start, stop = STAGES[s]
        for copy in sends[s]:
            copy.wait()
        low, high = base + start * rank, base + stop * rank
        fresh = raw[start:stop].astype(jnp.float32).reshape(high - low, width).astype(jnp.bfloat16)
        z[low:high, :] = fresh
        full = products(fresh, z[:high, :])
        groups = []
        for b in range(start, stop):
            near = full[(b - start) * rank:(b - start + 1) * rank, :4 * rank]
            folded = jnp.where(lane < base, fold(jnp.where(lane < base, near, 0.0)), near)
            if b == 0:
                middle = inner
            else:
                far = widen(full[(b - start) * rank:(b - start + 1) * rank, 4 * rank:4 * rank + rank * b])
                middle = pltpu.roll(far, rank, 1)
            groups.append(jnp.where((lane >= rank) & (lane < base), middle, folded))
            if b == batches - 1:
                groups.append(far)
        packed = jnp.concatenate(groups, axis=0)
        size = parts[s].shape[1]
        for j in range(members):
            parts[s][j] = packed[j * size:(j + 1) * size]

        @pl.loop(1, members)
        def _(step):
            target = peer(step)
            pltpu.make_async_remote_copy(
                src_ref=parts[s].at[target], dst_ref=landeds[s].at[step - 1],
                send_sem=rs_send.at[s], recv_sem=rs_recv.at[s], device_id=device(target), device_id_type=MESH,
            ).start()

    def gather_start(s):
        landed, crossed, total = landeds[s], crosseds[s], totals[s]
        pltpu.make_async_copy(landed, landed, rs_recv.at[s]).wait()
        mine = parts[s][me] + jnp.sum(landed[...], axis=0)
        if blocks > 1:
            crossed[0] = mine

            @pl.loop(1, blocks)
            def _(step):
                pltpu.make_async_remote_copy(
                    src_ref=crossed.at[0], dst_ref=crossed.at[step],
                    send_sem=x_send.at[s], recv_sem=x_recv.at[s], device_id=other(step), device_id_type=MESH,
                ).start()

            rest = crossed.at[pl.ds(1, blocks - 1)]
            pltpu.make_async_copy(rest, rest, x_recv.at[s]).wait()
            mine = jnp.sum(crossed[...], axis=0)
        total[me] = mine

        @pl.loop(1, members)
        def _(step):
            pltpu.make_async_remote_copy(
                src_ref=total.at[me], dst_ref=total.at[me],
                send_sem=ag_send.at[s], recv_sem=ag_recv.at[s], device_id=device(peer(step)), device_id_type=MESH,
            ).start()

    def gather_wait(s):
        most = totals[s].at[pl.ds(0, members - 1)]
        pltpu.make_async_copy(most, most, ag_recv.at[s]).wait()
        size = parts[s].shape[1]
        values = jnp.concatenate([totals[s][j] for j in range(members)], axis=0)
        return [values[g * rank:(g + 1) * rank] for g in range(size)]

    sub = lax.broadcasted_iota(jnp.int32, (rank, rank), 0)
    eye = sub == lane[:, :rank]
    coef = (lane == lax.broadcasted_iota(jnp.int32, (rank, 4 * rank), 0)).astype(jnp.float32)
    core = core_ref[...]
    spots = (3, 1, 2)

    def update(b, state, cross_raw, own):
        coef, energy, gram_basis = state
        diagonal = jnp.where(eye, own, 0.0)
        inverse_col = lax.rsqrt(jnp.sum(diagonal, axis=1, keepdims=True) + epsilon)
        inverse_row = lax.rsqrt(jnp.sum(diagonal, axis=0, keepdims=True) + epsilon)
        cross = mt(coef, cross_raw * inverse_col)
        first_ref[b] = cross
        total = cross + (cross - mm(gram_basis, cross))
        w1 = mm(energy, gram_basis) + mt(total, cross)
        w2 = mm(energy, cross) + mm(total, own * inverse_col * inverse_row)
        w1_energy = mm(w1, energy)
        square = w1_energy + mt(w2, total)
        placed = total * inverse_row
        kept = mm(energy, coef)
        if b < batches - 1:
            at = spots[b]
            strip = widen(jnp.concatenate([jnp.zeros((rank, at * rank), jnp.float32), placed], axis=1))
            kept = kept + strip
        inverse = eliminate(square)
        coef = mm(inverse, kept)
        if b == batches - 1:
            coef = (coef, mm(inverse, placed))
        else:
            gram_basis = mt(mm(inverse, square), inverse)
        n1 = mm(inverse, w1)
        n2 = mm(inverse, w2)
        energy = mt(mm(inverse, w1_energy), n1) + mt(n2, n2)
        return coef, energy, gram_basis

    reduce_start(0)
    reduce_start(1)
    gather_start(0)
    reduce_start(2)
    store_z = pltpu.make_async_copy(z, z_ref, z_sem)
    store_z.start()
    gather_start(1)
    sums, = gather_wait(0)
    state = (coef, mt(core, core), sums[:, rank:2 * rank])
    gather_start(2)
    state = update(0, state, sums, sums[:, base:])
    sums, = gather_wait(1)
    state = update(1, state, sums, sums[:, rank:2 * rank])
    sums, later, last = gather_wait(2)
    state = update(2, state, sums, sums[:, 2 * rank:base])
    (coef, coef_last), energy, _ = update(3, state, later, last[:, 2 * rank:base])
    energy_ref[...] = energy
    blocks_of = [coef[:, i * rank:(i + 1) * rank] for i in range(4)]
    wide = jnp.concatenate([blocks_of[0]] * 3 + [blocks_of[3], blocks_of[1], blocks_of[2], coef_last], axis=1)
    coef_ref[...] = wide
    for s in range(count):
        pltpu.make_async_copy(landeds[s], landeds[s], rs_send.at[s]).wait()
        if blocks > 1:
            rest = crosseds[s].at[pl.ds(1, blocks - 1)]
            pltpu.make_async_copy(rest, rest, x_send.at[s]).wait()
        most = totals[s].at[pl.ds(0, members - 1)]
        pltpu.make_async_copy(most, most, ag_send.at[s]).wait()
    store_z.wait()


def final_kernel(coef_ref, energy_ref, first_ref, z_ref, basis_out, core_out, first_out, z, z_sem):
    load = pltpu.make_async_copy(z_ref, z, z_sem)
    load.start()
    rank = energy_ref.shape[0]
    first_out[...] = first_ref[...]
    pieces = jnp.concatenate([p.astype(jnp.float32) for p in split(coef_ref[...])], axis=0).astype(jnp.bfloat16)
    core_out[...] = eliminate(energy_ref[...], want_lower=True)
    load.wait()
    wide = jnp.dot(pieces, z[...], preferred_element_type=jnp.float32)
    basis_out[...] = wide[:rank] + wide[rank:2 * rank] + wide[2 * rank:]


def solution(mesh):
    nrows, ngrp = mesh.shape["rows"], mesh.shape["grp"]

    def body(basis, core, snapshots):
        rank, width = basis.shape
        batches, cols, _ = snapshots.shape
        height = batches * cols * ngrp + 3 * rank
        members = BLOCK_ROWS * ngrp
        blocks = nrows // BLOCK_ROWS
        count = len(STAGES)
        sizes = [groups * rank // members for groups in GROUPS]
        vmem = pl.BlockSpec(memory_space=pltpu.VMEM)
        hbm = pl.BlockSpec(memory_space=pl.ANY)
        dma = pltpu.SemaphoreType.DMA
        buffers = [
            pltpu.VMEM((slots, size, 4 * rank), jnp.float32)
            for slots in (members, members - 1, blocks, members)
            for size in sizes
        ]
        z, coef, energy, firsts = pl.pallas_call(
            functools.partial(fused_kernel, nrows, ngrp),
            out_shape=(
                jax.ShapeDtypeStruct((height, width), jnp.bfloat16),
                jax.ShapeDtypeStruct((rank, height), jnp.float32),
                jax.ShapeDtypeStruct((rank, rank), jnp.float32),
                jax.ShapeDtypeStruct((batches, rank, rank), jnp.float32),
            ),
            in_specs=[hbm, vmem, hbm],
            out_specs=(hbm, vmem, vmem, vmem),
            scratch_shapes=[
                pltpu.VMEM((batches, ngrp, cols, width), jnp.bfloat16),
                pltpu.VMEM((rank, width), jnp.float32),
                pltpu.VMEM((height, width), jnp.bfloat16),
                *buffers,
                dma, dma, dma, dma((count, ngrp - 1)), dma((count, ngrp - 1)),
                *[dma((count,))] * 6,
            ],
            compiler_params=pltpu.CompilerParams(collective_id=0, has_side_effects=True),
        )(basis, core, snapshots)
        return pl.pallas_call(
            final_kernel,
            out_shape=(
                jax.ShapeDtypeStruct((rank, width), jnp.float32),
                jax.ShapeDtypeStruct((rank, rank), jnp.float32),
                jax.ShapeDtypeStruct((batches, rank, rank), jnp.float32),
            ),
            in_specs=[vmem, vmem, vmem, hbm],
            out_specs=(vmem, vmem, vmem),
            scratch_shapes=[pltpu.VMEM((height, width), jnp.bfloat16), dma],
        )(coef, energy, firsts, z)

    return jax.shard_map(
        body,
        mesh=mesh,
        in_specs=(P(None, ("rows", "grp")), P(), P(None, "grp", "rows")),
        out_specs=(P(None, ("rows", "grp")), P(), P()),
        check_vma=False,
    )
```

```python
import functools

import jax
import jax.numpy as jnp
from jax import lax
from jax.experimental import pallas as pl
from jax.experimental.pallas import tpu as pltpu
from jax.sharding import PartitionSpec as P

epsilon = 1e-06
BLOCK_ROWS = 8
STAGES = ((0, 1), (1, 2), (2, 4))
GROUPS = (1, 1, 3)
MESH = pl.DeviceIdType.MESH


def mm(left, right):
    return lax.dot_general(
        left, right, (((1,), (0,)), ((), ())), precision=lax.Precision.HIGHEST, preferred_element_type=jnp.float32
    )


def mt(left, right):
    return lax.dot_general(
        left, right, (((1,), (1,)), ((), ())), precision=lax.Precision.HIGHEST, preferred_element_type=jnp.float32
    )


def narrow(left, right):
    return jnp.dot(left.astype(jnp.bfloat16), right.astype(jnp.bfloat16), preferred_element_type=jnp.float32)


def split(x):
    high = x.astype(jnp.bfloat16)
    rest = x - high.astype(jnp.float32)
    mid = rest.astype(jnp.bfloat16)
    low = (rest - mid.astype(jnp.float32)).astype(jnp.bfloat16)
    return high, mid, low


def eliminate(matrix, want_lower=False):
    n = matrix.shape[0]
    tile = 8
    tiles = n // tile
    r = lax.broadcasted_iota(jnp.int32, (tile, n), 0)
    c = lax.broadcasted_iota(jnp.int32, (tile, n), 1)
    left = [matrix[t * tile:(t + 1) * tile] for t in range(tiles)]
    if want_lower:
        result = [jnp.zeros((tile, n), jnp.float32)] * tiles
    else:
        result = [(c == r + t * tile).astype(jnp.float32) for t in range(tiles)]
    for t in range(tiles):
        below = range(t, tiles)
        panel = [
            {u: jnp.broadcast_to(left[u][:, t * tile + j:t * tile + j + 1], (tile, n)) for u in below}
            for j in range(tile)
        ]
        scale = jnp.ones((tile, n), jnp.float32)
        for j in range(tile):
            k = t * tile + j
            column = panel[j]
            pivot = column[t][j:j + 1]
            inverse = 1.0 / pivot
            root = lax.rsqrt(pivot)
            if want_lower:
                for u in below:
                    keep = (c == k) & (r >= j) if u == t else c == k
                    result[u] = jnp.where(keep, column[u] * root, result[u])
            else:
                scale = jnp.where(r == j, root, scale)
            masked = {u: jnp.where(r > j, column[u], 0.0) if u == t else column[u] for u in below}
            for l in range(j + 1, tile):
                head = panel[l][t][j:j + 1]
                for u in below:
                    panel[l][u] = panel[l][u] - (masked[u] * head) * inverse
            top = left[t][j:j + 1] * inverse
            body = result[t][j:j + 1] * inverse
            for u in below:
                if t < tiles - 1:
                    left[u] = left[u] - masked[u] * top
                if not want_lower:
                    result[u] = result[u] - masked[u] * body
        if not want_lower:
            result[t] = result[t] * scale
    return jnp.concatenate(result, axis=0)


def fused_kernel(nrows, ngrp, basis_ref, core_ref, snap_ref, z_ref, coef_ref, energy_ref, first_ref, raw, basis_v, z, *scratch):
    count = len(STAGES)
    parts, landeds, crosseds, totals = (scratch[i * count:(i + 1) * count] for i in range(4))
    basis_sem, own_sem, z_sem, a2a_send, a2a_recv, rs_send, rs_recv, x_send, x_recv, ag_send, ag_recv = scratch[4 * count:]
    row, grp = lax.axis_index("rows"), lax.axis_index("grp")
    rank, width = basis_ref.shape
    batches, cols, _ = snap_ref.shape
    members = BLOCK_ROWS * ngrp
    blocks = nrows // BLOCK_ROWS
    block = row // BLOCK_ROWS
    me = (row % BLOCK_ROWS) * ngrp + grp

    def device(q):
        return (block * BLOCK_ROWS + q // ngrp, q % ngrp)

    def peer(step):
        return lax.rem(me + step, members)

    def other(step):
        return (lax.rem(block + step, blocks) * BLOCK_ROWS + row % BLOCK_ROWS, grp)

    def piece(g, start, stop):
        return snap_ref.at[start:stop, :, pl.ds(pl.multiple_of(g * width, 128), width)]

    load_basis = pltpu.make_async_copy(basis_ref, basis_v, basis_sem)
    load_basis.start()
    load_own = pltpu.make_async_copy(piece(grp, 0, batches), raw.at[:, grp], own_sem)
    load_own.start()

    barrier = pltpu.get_barrier_semaphore()

    @pl.loop(1, members)
    def _(step):
        pl.semaphore_signal(barrier, inc=1, device_id=device(peer(step)), device_id_type=MESH)

    if blocks > 1:

        @pl.loop(1, blocks)
        def _(step):
            pl.semaphore_signal(barrier, inc=1, device_id=other(step), device_id_type=MESH)

    pl.semaphore_wait(barrier, members - 1 + blocks - 1)

    sends = {}

    def exchange_start(s):
        start, stop = STAGES[s]
        stage = []
        for step in range(1, ngrp):
            target = lax.rem(grp + step, ngrp)
            copy = pltpu.make_async_remote_copy(
                src_ref=piece(target, start, stop), dst_ref=raw.at[start:stop, grp],
                send_sem=a2a_send.at[s, step - 1], recv_sem=a2a_recv.at[s, step - 1],
                device_id=(row, target), device_id_type=MESH,
            )
            copy.start()
            stage.append(copy)
        sends[s] = stage

    exchange_start(0)
    exchange_start(1)
    exchange_start(2)

    load_basis.wait()
    base = 3 * rank
    for i, value in enumerate(split(basis_v[...])):
        z[i * rank:(i + 1) * rank, :] = value
    load_own.wait()
    lane = lax.broadcasted_iota(jnp.int32, (rank, 4 * rank), 1)

    def products(left, right):
        return lax.dot_general(left, right, (((1,), (1,)), ((), ())), preferred_element_type=jnp.float32)

    def fold(x):
        return x + pltpu.roll(x, 3 * rank, 1) + pltpu.roll(x, 2 * rank, 1)

    def widen(x):
        missing = 4 * rank - x.shape[1]
        return x if missing == 0 else jnp.concatenate([x, jnp.zeros((rank, missing), jnp.float32)], axis=1)

    inner = products(z[:base, :], z[:base, :])
    inner = widen(inner[:rank] + inner[rank:2 * rank] + inner[2 * rank:])
    inner = pltpu.roll(fold(inner), rank, 1)

    def reduce_start(s):
        start, stop = STAGES[s]
        for copy in sends[s]:
            copy.wait()
        low, high = base + start * rank, base + stop * rank
        fresh = raw[start:stop].astype(jnp.float32).reshape(high - low, width).astype(jnp.bfloat16)
        z[low:high, :] = fresh
        full = products(fresh, z[:high, :])
        groups = []
        for b in range(start, stop):
            near = full[(b - start) * rank:(b - start + 1) * rank, :4 * rank]
            folded = jnp.where(lane < base, fold(jnp.where(lane < base, near, 0.0)), near)
            if b == 0:
                middle = inner
            else:
                far = widen(full[(b - start) * rank:(b - start + 1) * rank, 4 * rank:4 * rank + rank * b])
                middle = pltpu.roll(far, rank, 1)
            groups.append(jnp.where((lane >= rank) & (lane < base), middle, folded))
            if b == batches - 1:
                groups.append(far)
        packed = jnp.concatenate(groups, axis=0)
        size = parts[s].shape[1]
        for j in range(members):
            parts[s][j] = packed[j * size:(j + 1) * size]

        @pl.loop(1, members)
        def _(step):
            target = peer(step)
            pltpu.make_async_remote_copy(
                src_ref=parts[s].at[target], dst_ref=landeds[s].at[step - 1],
                send_sem=rs_send.at[s], recv_sem=rs_recv.at[s], device_id=device(target), device_id_type=MESH,
            ).start()

    def gather_start(s):
        landed, crossed, total = landeds[s], crosseds[s], totals[s]
        pltpu.make_async_copy(landed, landed, rs_recv.at[s]).wait()
        mine = parts[s][me] + jnp.sum(landed[...], axis=0)
        if blocks > 1:
            crossed[0] = mine

            @pl.loop(1, blocks)
            def _(step):
                pltpu.make_async_remote_copy(
                    src_ref=crossed.at[0], dst_ref=crossed.at[step],
                    send_sem=x_send.at[s], recv_sem=x_recv.at[s], device_id=other(step), device_id_type=MESH,
                ).start()

            rest = crossed.at[pl.ds(1, blocks - 1)]
            pltpu.make_async_copy(rest, rest, x_recv.at[s]).wait()
            mine = jnp.sum(crossed[...], axis=0)
        total[me] = mine

        @pl.loop(1, members)
        def _(step):
            pltpu.make_async_remote_copy(
                src_ref=total.at[me], dst_ref=total.at[me],
                send_sem=ag_send.at[s], recv_sem=ag_recv.at[s], device_id=device(peer(step)), device_id_type=MESH,
            ).start()

    def gather_wait(s):
        most = totals[s].at[pl.ds(0, members - 1)]
        pltpu.make_async_copy(most, most, ag_recv.at[s]).wait()
        size = parts[s].shape[1]
        values = jnp.concatenate([totals[s][j] for j in range(members)], axis=0)
        return [values[g * rank:(g + 1) * rank] for g in range(size)]

    sub = lax.broadcasted_iota(jnp.int32, (rank, rank), 0)
    eye = sub == lane[:, :rank]
    coef = (lane == lax.broadcasted_iota(jnp.int32, (rank, 4 * rank), 0)).astype(jnp.float32)
    identity = eye.astype(jnp.float32)
    core = core_ref[...]
    spots = (3, 1, 2)

    def update(b, state, cross_raw, own):
        coef, energy, excess = state
        diagonal = jnp.where(eye, own, 0.0)
        inverse_col = lax.rsqrt(jnp.sum(diagonal, axis=1, keepdims=True) + epsilon)
        inverse_row = lax.rsqrt(jnp.sum(diagonal, axis=0, keepdims=True) + epsilon)
        cross = mt(coef, cross_raw * inverse_col)
        first_ref[b] = cross
        total = cross - narrow(excess, cross)
        w1 = energy + narrow(energy, excess) + mt(total, cross)
        w2 = mm(energy, cross) + mm(total, own * inverse_col * inverse_row)
        w1_energy = mm(w1, energy)
        square = w1_energy + mt(w2, total)
        placed = total * inverse_row
        kept = mm(energy, coef)
        if b < batches - 1:
            at = spots[b]
            strip = widen(jnp.concatenate([jnp.zeros((rank, at * rank), jnp.float32), placed], axis=1))
            kept = kept + strip
        bundle = jnp.concatenate([w1, w2, w1_energy, square], axis=1)
        inverse = eliminate(square)
        coef = mm(inverse, kept)
        bundle = mm(inverse, bundle)
        if b == batches - 1:
            coef = (coef, mm(inverse, placed))
        else:
            excess = mt(bundle[:, base:], inverse) - identity
        n2 = bundle[:, rank:2 * rank]
        energy = mt(bundle[:, 2 * rank:base], bundle[:, :rank]) + mt(n2, n2)
        return coef, energy, excess

    reduce_start(0)
    reduce_start(1)
    gather_start(0)
    reduce_start(2)
    store_z = pltpu.make_async_copy(z, z_ref, z_sem)
    store_z.start()
    gather_start(1)
    sums, = gather_wait(0)
    state = (coef, mt(core, core), sums[:, rank:2 * rank] - identity)
    gather_start(2)
    state = update(0, state, sums, sums[:, base:])
    sums, = gather_wait(1)
    state = update(1, state, sums, sums[:, rank:2 * rank])
    sums, later, last = gather_wait(2)
    state = update(2, state, sums, sums[:, 2 * rank:base])
    (coef, coef_last), energy, _ = update(3, state, later, last[:, 2 * rank:base])
    energy_ref[...] = energy
    blocks_of = [coef[:, i * rank:(i + 1) * rank] for i in range(4)]
    wide = jnp.concatenate([blocks_of[0]] * 3 + [blocks_of[3], blocks_of[1], blocks_of[2], coef_last], axis=1)
    coef_ref[...] = wide
    for s in range(count):
        pltpu.make_async_copy(landeds[s], landeds[s], rs_send.at[s]).wait()
        if blocks > 1:
            rest = crosseds[s].at[pl.ds(1, blocks - 1)]
            pltpu.make_async_copy(rest, rest, x_send.at[s]).wait()
        most = totals[s].at[pl.ds(0, members - 1)]
        pltpu.make_async_copy(most, most, ag_send.at[s]).wait()
    store_z.wait()


def final_kernel(coef_ref, energy_ref, first_ref, z_ref, basis_out, core_out, first_out, z, z_sem):
    load = pltpu.make_async_copy(z_ref, z, z_sem)
    load.start()
    rank = energy_ref.shape[0]
    first_out[...] = first_ref[...]
    pieces = jnp.concatenate([p.astype(jnp.float32) for p in split(coef_ref[...])], axis=0).astype(jnp.bfloat16)
    load.wait()
    wide = jnp.dot(pieces, z[...], preferred_element_type=jnp.float32)
    core_out[...] = eliminate(energy_ref[...], want_lower=True)
    basis_out[...] = wide[:rank] + wide[rank:2 * rank] + wide[2 * rank:]


def solution(mesh):
    nrows, ngrp = mesh.shape["rows"], mesh.shape["grp"]

    def body(basis, core, snapshots):
        rank, width = basis.shape
        batches, cols, _ = snapshots.shape
        height = batches * cols * ngrp + 3 * rank
        members = BLOCK_ROWS * ngrp
        blocks = nrows // BLOCK_ROWS
        count = len(STAGES)
        sizes = [groups * rank // members for groups in GROUPS]
        vmem = pl.BlockSpec(memory_space=pltpu.VMEM)
        hbm = pl.BlockSpec(memory_space=pl.ANY)
        dma = pltpu.SemaphoreType.DMA
        buffers = [
            pltpu.VMEM((slots, size, 4 * rank), jnp.float32)
            for slots in (members, members - 1, blocks, members)
            for size in sizes
        ]
        z, coef, energy, firsts = pl.pallas_call(
            functools.partial(fused_kernel, nrows, ngrp),
            out_shape=(
                jax.ShapeDtypeStruct((height, width), jnp.bfloat16),
                jax.ShapeDtypeStruct((rank, height), jnp.float32),
                jax.ShapeDtypeStruct((rank, rank), jnp.float32),
                jax.ShapeDtypeStruct((batches, rank, rank), jnp.float32),
            ),
            in_specs=[hbm, vmem, hbm],
            out_specs=(hbm, vmem, vmem, vmem),
            scratch_shapes=[
                pltpu.VMEM((batches, ngrp, cols, width), jnp.bfloat16),
                pltpu.VMEM((rank, width), jnp.float32),
                pltpu.VMEM((height, width), jnp.bfloat16),
                *buffers,
                dma, dma, dma, dma((count, ngrp - 1)), dma((count, ngrp - 1)),
                *[dma((count,))] * 6,
            ],
            compiler_params=pltpu.CompilerParams(collective_id=0, has_side_effects=True),
        )(basis, core, snapshots)
        return pl.pallas_call(
            final_kernel,
            out_shape=(
                jax.ShapeDtypeStruct((rank, width), jnp.float32),
                jax.ShapeDtypeStruct((rank, rank), jnp.float32),
                jax.ShapeDtypeStruct((batches, rank, rank), jnp.float32),
            ),
            in_specs=[vmem, vmem, vmem, hbm],
            out_specs=(vmem, vmem, vmem),
            scratch_shapes=[pltpu.VMEM((height, width), jnp.bfloat16), dma],
        )(coef, energy, firsts, z)

    return jax.shard_map(
        body,
        mesh=mesh,
        in_specs=(P(None, ("rows", "grp")), P(), P(None, "grp", "rows")),
        out_specs=(P(None, ("rows", "grp")), P(), P()),
        check_vma=False,
    )
```
